32 devices in a mesh: dp: 8 (over y, x, core), tensor: 4 (over z).
Axes of the slice: x: 2, y: 2, z: 4, core: 2. Of those that a mesh axis runs over, the one named last changes fastest.
Arguments:
- features: bfloat16 [2048, 1024], P(('dp', 'tensor')), may hold values from -6 to 6
- click: int32 [2048], P(('dp', 'tensor')), may hold values 0 or 1
- convert: int32 [2048], P(('dp', 'tensor')), may hold values 0 or 1
- w1: bfloat16 [1024, 2, 4096], P('dp', None, 'tensor'), may hold values from -0.1875 to 0.1875
- b1: float32 [2, 4096], P(None, 'tensor'), may hold values from -4 to 4
- w2: bfloat16 [2, 4096], P(None, 'tensor'), may hold values from -0.1875 to 0.1875
Outputs:
- sample_loss: float32 [2048], P(('dp', 'tensor'))
- grad_features: bfloat16 [2048, 1024], P(('dp', 'tensor'))
- grad_w1: float32 [1024, 2, 4096], P('dp', None, 'tensor')
- grad_b1: float32 [2, 4096], P(None, 'tensor')
- grad_w2: float32 [2, 4096], P(None, 'tensor')
The draws below stay inside these ranges and needn't reach their ends.
All inputs are finite; a program needn't handle non-finite values. No bound on the sum of `click` or of `convert` on one device may be relied on, other than what follows from the above.
Results may differ from the reference program's by a relative error of at most 0.025.
Values may be sent and summed in bfloat16 or wider, within the bound.
A program may use at most 64 MiB of HBM per device.

```python
import math
import jax
import jax.numpy as jnp
from jax import lax

D = 1024
H = 4096
SAMPLES = 2048


def plant(array, own_key, low, top_value):
    dims = array.shape
    place = [jax.random.randint(jax.random.fold_in(own_key, axis), (), 0, dims[axis]) for axis in range(len(dims))]
    array = array.at[tuple(place)].set(low)
    longest = dims.index(max(dims))
    place[longest] = (place[longest] + 1) % dims[longest]
    return array.at[tuple(place)].set(top_value)


def spiked(entries, own_key, source, target, shards_of, factor):
    owner, partner = [(jnp.arange(entries.shape[position]) // (entries.shape[position] // shards_of)).reshape([-1 if axis == position else 1 for axis in range(entries.ndim)]) for position in (source, target)]
    chosen = jax.random.permutation(own_key, shards_of)[partner]
    strong = (owner == chosen) | (owner == (partner + shards_of // 2) % shards_of)
    return jnp.where(strong, factor * entries, entries)


def block_scale(stream_key, extent, pieces, least, top_value):
    factor_of, own = 1.0, jax.random.fold_in(stream_key, 6)
    for dim, parts in pieces:
        heights = jnp.exp(jax.random.uniform(jax.random.fold_in(own, dim), (parts,), jnp.float32, least / len(pieces), top_value / len(pieces)))
        factor_of = factor_of * jnp.repeat(heights, extent[dim] // parts).reshape([-1 if axis == dim else 1 for axis in range(len(extent))])
    return factor_of


def normal_values(stream_key, dims, scale, most, cuts=(), held_as=jnp.bfloat16):
    drawn = jax.random.normal(stream_key, dims, jnp.float32) * scale
    if len(cuts) > 0:
        drawn = block_scale(stream_key, dims, cuts, -0.22, 0.18) * drawn
    return jnp.clip(drawn, min=-most, max=most).astype(held_as)


def bell_draw_with(key, extent, scale, bound, cuts, heavy, held_as=jnp.bfloat16):
    values = scale * jax.random.normal(key, extent, jnp.float32)
    if cuts:
        values = values * block_scale(key, extent, cuts, -0.22, 0.18)
    return jnp.clip(spiked(values, jax.random.fold_in(key, 3), *heavy), -bound, bound).astype(held_as)


def setup_inputs(seed: int = 0) -> dict:
    key_list = jax.random.split(jax.random.key(seed), 7)
    features = bell_draw_with(key_list[0], (SAMPLES, D), 1.0, 6.0, ((0, 32),), (0, 1, 32, 2.75))
    click = plant((jax.random.randint(key_list[1], (SAMPLES,), 0, 3) < 1).astype(jnp.int32), jax.random.fold_in(key_list[1], 1), 0, 1)
    convert = plant((jax.random.randint(key_list[2], (SAMPLES,), 0, 2) < 1).astype(jnp.int32), jax.random.fold_in(key_list[2], 1), 0, 1)
    w1 = normal_values(key_list[3], (D, 2, H), D ** -0.5, 0.1875, ((0, 8), (2, 4)))
    b1 = normal_values(key_list[4], (2, H), 0.7, 4.0, ((1, 4),), jnp.float32)
    w2 = normal_values(key_list[5], (2, H), (H // 4) ** -0.5, 0.1875, ((1, 4),))
    return {"features": features, "click": click, "convert": convert, "w1": w1, "b1": b1, "w2": w2}


def sample_loss_fn(logits, click, convert):
    first = logits[:, 0]
    second = logits[:, 1]
    label_y = click.astype(jnp.float32)
    label_z = (click * convert).astype(jnp.float32)
    rest = jnp.log(jax.nn.sigmoid(-first) + jax.nn.sigmoid(first) * jax.nn.sigmoid(-second))
    click_part = label_y * jax.nn.log_sigmoid(first) + (1.0 - label_y) * jax.nn.log_sigmoid(-first)
    both_part = label_z * (jax.nn.log_sigmoid(first) + jax.nn.log_sigmoid(second)) + (1.0 - label_z) * rest
    return -click_part - both_part

def reference(features, click, convert, w1, b1, w2):
    total, width = features.shape
    hidden_units = w1.shape[2]
    block = min(total, 4096)
    blocks = total // block
    w_flat = w1.reshape(width, 2 * hidden_units)
    w2f = w2.astype(jnp.float32)

    def step(carry, inputs):
        acc_w1, acc_b1, acc_w2 = carry
        rows, clicks, converts = inputs
        pre = jnp.dot(rows, w_flat, preferred_element_type=jnp.float32).reshape(block, 2, hidden_units) + b1[None]
        hidden = jnp.maximum(pre, 0.0).astype(jnp.bfloat16)
        logits = lax.optimization_barrier(jnp.sum(hidden.astype(jnp.float32) * w2f[None], axis=2))
        losses, pullback = jax.vjp(lambda value: sample_loss_fn(value, clicks, converts), logits)
        slope = pullback(jnp.ones_like(losses))[0]
        dhidden = jnp.where(pre > 0.0, slope[:, :, None] * w2f[None], 0.0).astype(jnp.bfloat16)
        d_flat = dhidden.reshape(block, 2 * hidden_units)
        grad_rows = jnp.dot(d_flat, w_flat.T, preferred_element_type=jnp.float32).astype(jnp.bfloat16)
        acc_w1 = acc_w1 + jnp.dot(rows.T, d_flat, preferred_element_type=jnp.float32).reshape(width, 2, hidden_units)
        acc_b1 = acc_b1 + lax.optimization_barrier(jnp.sum(dhidden.astype(jnp.float32), axis=0))
        acc_w2 = acc_w2 + lax.optimization_barrier(jnp.sum(slope[:, :, None] * hidden.astype(jnp.float32), axis=0))
        return ((acc_w1, acc_b1, acc_w2), (losses, grad_rows))
    start = (jnp.zeros((width, 2, hidden_units), jnp.float32), jnp.zeros((2, hidden_units), jnp.float32), jnp.zeros((2, hidden_units), jnp.float32))
    carry, outs = lax.scan(step, start, (features.reshape(blocks, block, width), click.reshape(blocks, block), convert.reshape(blocks, block)))
    scale = 1.0 / math.sqrt(total)
    losses = outs[0].reshape(total)
    grad_features = outs[1].reshape(total, width)
    return (losses, grad_features, carry[0] * scale, carry[1] * scale, carry[2] * scale)
```

```python
import functools
import math

import jax
import jax.numpy as jnp
from jax import lax
from jax.experimental import pallas as pl
from jax.experimental.pallas import tpu as pltpu
from jax.sharding import PartitionSpec as P

MESH = pl.DeviceIdType.MESH
F32 = jnp.float32
BF16 = jnp.bfloat16


def log_sigmoid(x):
    return jnp.minimum(x, 0.0) - jnp.log(1.0 + jnp.exp(-jnp.abs(x)))


def first_phase(rel, order):
    for phase, mask in enumerate(order):
        if rel & mask:
            return phase
    return len(order)


def kernel(
    dp, tp, scale, f_ref, lab_ref, w1_ref, b1_ref, w2_ref,
    loss_ref, gf_ref, gw_ref, small_ref,
    weights, feats, feats_t, labels, logit_out, logit_in, pre, hid, dh,
    out_buf, in_buf, rows_out, rows_in, sums,
    wg_send, wg_recv, ws_send, ws_recv, t_send, t_recv, b_send, b_recv,
):
    me = lax.axis_index("dp")
    mt = lax.axis_index("tensor")
    rows, units = w1_ref.shape[1], w1_ref.shape[2]
    own_count, width = f_ref.shape
    count = own_count * tp
    tile = min(256, units)
    tiles = units // tile
    high = [1 << bit for bit in range(1, dp.bit_length() - 1)]
    orders = (high, high[::-1])

    def flip(mask):
        return me + mask - 2 * (me & mask)

    def flip_rel(rel):
        out = me
        bit = 1
        while bit <= rel:
            if rel & bit:
                out = out + bit - 2 * (lax.rem(me // bit, 2) * bit)
            bit *= 2
        return out

    def peer(rel):
        return flip_rel(rel)

    barrier = pltpu.get_barrier_semaphore()
    for j in range(1, dp):
        pl.semaphore_signal(barrier, inc=1, device_id={"dp": lax.rem(me + j, dp)}, device_id_type=MESH)
    for j in range(1, tp):
        pl.semaphore_signal(barrier, inc=1, device_id={"tensor": lax.rem(mt + j, tp)}, device_id_type=MESH)
    pl.semaphore_wait(barrier, dp + tp - 2)

    def block_rows(rel):
        return pl.ds(pl.multiple_of(flip_rel(rel) * rows, rows), rows)

    def gather_copy(t, rel, mask):
        place = weights.at[t, block_rows(rel)]
        src = w1_ref.at[t] if rel == 0 else place
        key = rel ^ mask
        return pltpu.make_async_remote_copy(
            src_ref=src, dst_ref=place, send_sem=wg_send.at[t, key], recv_sem=wg_recv.at[t, key],
            device_id={"dp": peer(mask)}, device_id_type=MESH,
        )

    def to_tensor(j, kind, src, dst):
        return pltpu.make_async_remote_copy(
            src_ref=src, dst_ref=dst, send_sem=t_send.at[kind, j], recv_sem=t_recv.at[kind, j],
            device_id={"tensor": lax.rem(mt + j, tp)}, device_id_type=MESH,
        )

    pending = []
    gathers = {}

    def launch(t, rel, mask):
        copy = gather_copy(t, rel, mask)
        copy.start()
        gathers[t, rel ^ mask] = copy

    for phase in range(len(high)):
        for t in range(2):
            launch(t, 0, orders[t][phase])
    own_rows = pl.ds(pl.multiple_of(mt * own_count, own_count), own_count)
    feat_copies = [to_tensor(j, 0, f_ref, feats.at[own_rows]) for j in range(1, tp)]
    lab_copies = [to_tensor(j, 1, lab_ref, labels.at[mt]) for j in range(1, tp)]
    for copy in feat_copies + lab_copies:
        copy.start()
    for t in range(2):
        launch(t, 0, 1)
    feats[own_rows, :] = f_ref[...]
    labels[mt] = lab_ref[...]
    for t in range(2):
        weights[t, block_rows(0), :] = w1_ref[t]

    for phase in range(len(high)):
        arriving = []
        for t in range(2):
            held = [0]
            for mask in orders[t][:phase]:
                held = held + [rel ^ mask for rel in held]
            arriving.append([rel ^ orders[t][phase] for rel in held])
        for step in range(len(arriving[0])):
            for t in range(2):
                rel = arriving[t][step]
                gathers[t, rel].wait_recv()
                for mask in orders[t][phase + 1:]:
                    launch(t, rel, mask)
                launch(t, rel, 1)
        if phase == 0:
            for copy in feat_copies + lab_copies:
                copy.wait_recv()
            feats_t[...] = feats[...].T
    label_sum = labels[0]
    for j in range(1, tp):
        label_sum = label_sum + labels[j]
    label_y = label_sum[0:1]
    label_z = label_sum[1:2]
    for t in range(2):
        for rel in range(1, dp, 2):
            gathers[t, rel].wait_recv()

    for t in range(2):
        def forward(j, total, t=t):
            cols = pl.ds(pl.multiple_of(j * tile, tile), tile)
            value = jnp.dot(feats[...], weights[t, :, cols], preferred_element_type=F32) + b1_ref[t:t + 1, cols]
            pre[t, :, cols] = value
            hidden = jnp.maximum(value, 0.0).astype(BF16)
            hid[t, :, cols] = hidden
            row = jnp.broadcast_to(w2_ref[t:t + 1, cols], (16, tile)).astype(BF16)
            return total + lax.dot_general(row, hidden, (((1,), (1,)), ((), ())), preferred_element_type=F32)

        total = lax.fori_loop(0, tiles, forward, jnp.zeros((16, count), F32))
        logit_out[t] = total[0:8]
    logit_copies = [to_tensor(j, 2, logit_out, logit_in.at[mt]) for j in range(1, tp)]
    for copy in logit_copies:
        copy.start()
    logit_in[mt] = logit_out[...]
    for copy in logit_copies:
        copy.wait_recv()
    first = logit_in[0, 0]
    second = logit_in[0, 1]
    for j in range(1, tp):
        first = first + logit_in[j, 0]
        second = second + logit_in[j, 1]
    sa, na = jax.nn.sigmoid(first), jax.nn.sigmoid(-first)
    sb, nb = jax.nn.sigmoid(second), jax.nn.sigmoid(-second)
    q = na + sa * nb
    rest = jnp.log(q)
    la, lna, lb = log_sigmoid(first), log_sigmoid(-first), log_sigmoid(second)
    loss_ref[...] = -(label_y * la + (1.0 - label_y) * lna) - (label_z * (la + lb) + (1.0 - label_z) * rest)
    shared = (1.0 - label_z) * (sa * sb / q)
    slopes = (
        -(label_y * na - (1.0 - label_y) * sa) - (label_z * na - shared * na),
        -(label_z * nb - shared * nb),
    )
    columns = [jnp.transpose(slope)[:, 0:1] for slope in slopes]
    for t in range(2):
        for j in range(tiles):
            cols = pl.ds(j * tile, tile)
            value = columns[t] * w2_ref[t:t + 1, cols].astype(F32)
            dh[t, :, cols] = jnp.where(pre[t, :, cols] > 0.0, value, 0.0).astype(BF16)

    def grad_block(t, rel):
        return jnp.dot(feats_t[block_rows(rel), :], dh[t], preferred_element_type=F32)

    scatters = {}

    def send_sum(t, key, mask, value):
        out_buf[t, key] = value.astype(BF16)
        copy = pltpu.make_async_remote_copy(
            src_ref=out_buf.at[t, key], dst_ref=in_buf.at[t, key],
            send_sem=ws_send.at[t, key], recv_sem=ws_recv.at[t, key],
            device_id={"dp": peer(mask)}, device_id_type=MESH,
        )
        copy.start()
        scatters[t, key] = copy

    ranked = []
    for t in range(2):
        ranked.append(sorted(range(0, dp, 2), key=lambda rel: (first_phase(rel, orders[t]), -bin(rel).count("1"))))
    for step in range(dp // 2):
        for t in range(2):
            rel = ranked[t][step]
            send_sum(t, rel ^ 1, 1, grad_block(t, rel ^ 1))

    def reduced(t, rel):
        value = grad_block(t, rel)
        keys = [rel ^ 1] + [rel ^ mask for mask in orders[t][:first_phase(rel, orders[t])]]
        for key in keys:
            scatters_recv(t, key)
            value = value + in_buf[t, key].astype(F32)
        return value

    def scatters_recv(t, key):
        pltpu.make_async_remote_copy(
            src_ref=out_buf.at[t, key], dst_ref=in_buf.at[t, key],
            send_sem=ws_send.at[t, key], recv_sem=ws_recv.at[t, key],
            device_id={"dp": peer(1)}, device_id_type=MESH,
        ).wait_recv()

    def process(step):
        for t in range(2):
            rel = ranked[t][step]
            if rel:
                mask = orders[t][first_phase(rel, orders[t])]
                send_sum(t, rel, mask, reduced(t, rel))
            else:
                gw_ref[t] = reduced(t, 0) * scale

    early = dp // 4
    for step in range(early):
        process(step)

    def backward(j, carry):
        place = pl.ds(pl.multiple_of(j * tile, tile), tile)
        value = jnp.zeros((count, tile), F32)
        for t in range(2):
            value = value + lax.dot_general(
                dh[t], weights[t, place, :], (((1,), (1,)), ((), ())), preferred_element_type=F32
            )
        rows_out[:, place] = value.astype(BF16)
        return carry

    lax.fori_loop(0, width // tile, backward, 0)

    def rows_of(index):
        return pl.ds(pl.multiple_of(index * own_count, own_count), own_count)

    row_copies = [
        to_tensor(j, 3, rows_out.at[rows_of(lax.rem(mt + j, tp))], rows_in.at[j]) for j in range(1, tp)
    ]
    for copy in row_copies:
        copy.start()

    for t in range(2):
        for j in range(tiles):
            cols = pl.ds(j * tile, tile)
            sums[me, t:t + 1, cols] = jnp.sum(dh[t, :, cols].astype(F32), axis=0, keepdims=True)
            sums[me, 2 + t:3 + t, cols] = jnp.sum(columns[t] * hid[t, :, cols].astype(F32), axis=0, keepdims=True)
    sum_copies = []
    for j in range(1, dp):
        copy = pltpu.make_async_remote_copy(
            src_ref=sums.at[me], dst_ref=sums.at[me], send_sem=b_send.at[j], recv_sem=b_recv.at[j],
            device_id={"dp": lax.rem(me + j, dp)}, device_id_type=MESH,
        )
        copy.start()
        sum_copies.append(copy)

    for step in range(early, dp // 2 - 1):
        process(step)
    for copy in row_copies:
        copy.wait_recv()
    own = rows_out[rows_of(mt), :].astype(F32)
    for j in range(1, tp):
        own = own + rows_in[j].astype(F32)
    gf_ref[...] = own.astype(BF16)
    for copy in sum_copies:
        copy.wait_recv()
    total = sums[0]
    for j in range(1, dp):
        total = total + sums[j]
    small_ref[...] = total * scale
    process(dp // 2 - 1)
    for copy in list(gathers.values()) + feat_copies + lab_copies + logit_copies + list(scatters.values()) + row_copies + sum_copies:
        copy.wait_send()


def solution(mesh):
    dp, tp = mesh.shape["dp"], mesh.shape["tensor"]

    def local(features, click, convert, w1, b1, w2):
        own_count, width = features.shape
        rows, _, units = w1.shape
        count = own_count * tp
        scale = 1.0 / math.sqrt(own_count * dp * tp)
        offset = lax.axis_index("tensor") * own_count
        both = jnp.stack([click, click * convert], axis=0).astype(F32)
        lab = lax.dynamic_update_slice(jnp.zeros((8, count), F32), both, (0, offset))
        vmem = pl.BlockSpec(memory_space=pltpu.VMEM)
        loss, gf, gw, small = pl.pallas_call(
            functools.partial(kernel, dp, tp, scale),
            out_shape=(
                jax.ShapeDtypeStruct((8, count), F32),
                jax.ShapeDtypeStruct((own_count, width), BF16),
                jax.ShapeDtypeStruct((2, rows, units), F32),
                jax.ShapeDtypeStruct((4, units), F32),
            ),
            in_specs=[vmem] * 5,
            out_specs=(vmem,) * 4,
            scratch_shapes=[
                pltpu.VMEM((2, width, units), BF16),
                pltpu.VMEM((count, width), BF16),
                pltpu.VMEM((width, count), BF16),
                pltpu.VMEM((tp, 8, count), F32),
                pltpu.VMEM((2, 8, count), F32),
                pltpu.VMEM((tp, 2, 8, count), F32),
                pltpu.VMEM((2, count, units), F32),
                pltpu.VMEM((2, count, units), BF16),
                pltpu.VMEM((2, count, units), BF16),
                pltpu.VMEM((2, dp, rows, units), BF16),
                pltpu.VMEM((2, dp, rows, units), BF16),
                pltpu.VMEM((count, width), BF16),
                pltpu.VMEM((tp, own_count, width), BF16),
                pltpu.VMEM((dp, 4, units), F32),
                pltpu.SemaphoreType.DMA((2, dp)),
                pltpu.SemaphoreType.DMA((2, dp)),
                pltpu.SemaphoreType.DMA((2, dp)),
                pltpu.SemaphoreType.DMA((2, dp)),
                pltpu.SemaphoreType.DMA((4, tp)),
                pltpu.SemaphoreType.DMA((4, tp)),
                pltpu.SemaphoreType.DMA((dp,)),
                pltpu.SemaphoreType.DMA((dp,)),
            ],
            compiler_params=pltpu.CompilerParams(
                collective_id=0, has_side_effects=True, vmem_limit_bytes=48 * 1024 * 1024
            ),
        )(features, lab, jnp.transpose(w1, (1, 0, 2)), b1, w2)
        losses = lax.dynamic_slice(loss, (0, offset), (1, own_count))[0]
        return (losses, gf, jnp.transpose(gw, (1, 0, 2)), small[0:2], small[2:4])

    return jax.shard_map(
        local,
        mesh=mesh,
        in_specs=(
            P(("dp", "tensor"), None),
            P(("dp", "tensor")),
            P(("dp", "tensor")),
            P("dp", None, "tensor"),
            P(None, "tensor"),
            P(None, "tensor"),
        ),
        out_specs=(
            P(("dp", "tensor")),
            P(("dp", "tensor"), None),
            P("dp", None, "tensor"),
            P(None, "tensor"),
            P(None, "tensor"),
        ),
        check_vma=False,
    )
```

```python
import functools
import math

import jax
import jax.numpy as jnp
from jax import lax
from jax.experimental import pallas as pl
from jax.experimental.pallas import tpu as pltpu
from jax.sharding import PartitionSpec as P

MESH = pl.DeviceIdType.MESH
F32 = jnp.float32
BF16 = jnp.bfloat16


def log_sigmoid(x):
    return jnp.minimum(x, 0.0) - jnp.log1p(jnp.exp(-jnp.abs(x)))


def first_phase(rel, order):
    for phase, mask in enumerate(order):
        if rel & mask:
            return phase
    return len(order)


def kernel(
    dp, tp, scale, f_ref, click_ref, convert_ref, w1_ref, b1_ref, w2_ref,
    loss_ref, gf_ref, gw_ref, small_ref,
    weights, feats, feats_t, labels, logit_out, logit_in, pre, hid, dh,
    out_buf, in_buf, rows_out, rows_in, sums, sums_in,
    wg_send, wg_recv, ws_send, ws_recv, t_send, t_recv, b_send, b_recv,
):
    me = lax.axis_index("dp")
    mt = lax.axis_index("tensor")
    rows, units = w1_ref.shape[1], w1_ref.shape[2]
    own_count, width = f_ref.shape
    count = own_count * tp
    tile = min(256, units)
    tiles = units // tile
    high = [1 << bit for bit in range(1, dp.bit_length() - 1)]
    orders = (high, high[::-1])

    def flip(mask):
        return me + mask - 2 * (me & mask)

    def flip_rel(rel):
        out = me
        bit = 1
        while bit <= rel:
            if rel & bit:
                out = out + bit - 2 * (lax.rem(me // bit, 2) * bit)
            bit *= 2
        return out

    def peer(rel):
        return flip_rel(rel)

    barrier = pltpu.get_barrier_semaphore()
    for j in range(1, dp):
        pl.semaphore_signal(barrier, inc=1, device_id={"dp": lax.rem(me + j, dp)}, device_id_type=MESH)
    for j in range(1, tp):
        pl.semaphore_signal(barrier, inc=1, device_id={"tensor": lax.rem(mt + j, tp)}, device_id_type=MESH)
    pl.semaphore_wait(barrier, dp + tp - 2)

    def block_rows(rel):
        return pl.ds(pl.multiple_of(flip_rel(rel) * rows, rows), rows)

    def gather_copy(t, rel, mask):
        place = weights.at[t, block_rows(rel)]
        src = w1_ref.at[t] if rel == 0 else place
        key = rel ^ mask
        return pltpu.make_async_remote_copy(
            src_ref=src, dst_ref=place, send_sem=wg_send.at[t, key], recv_sem=wg_recv.at[t, key],
            device_id={"dp": peer(mask)}, device_id_type=MESH,
        )

    def to_tensor(j, kind, src, dst):
        return pltpu.make_async_remote_copy(
            src_ref=src, dst_ref=dst, send_sem=t_send.at[kind, j], recv_sem=t_recv.at[kind, j],
            device_id={"tensor": lax.rem(mt + j, tp)}, device_id_type=MESH,
        )

    pending = []
    gathers = {}

    def launch(t, rel, mask):
        copy = gather_copy(t, rel, mask)
        copy.start()
        gathers[t, rel ^ mask] = copy

    for phase in range(len(high)):
        for t in range(2):
            launch(t, 0, orders[t][phase])
    own_rows = pl.ds(pl.multiple_of(mt * own_count, own_count), own_count)
    feat_copies = [to_tensor(j, 0, f_ref, feats.at[own_rows]) for j in range(1, tp)]
    lab_copies = [to_tensor(j, 1, labels.at[mt], labels.at[mt]) for j in range(1, tp)]
    click = click_ref[...].astype(F32)
    both = click * convert_ref[...].astype(F32)
    mine = lax.broadcasted_iota(jnp.int32, (1, count), 1) // own_count == mt
    for row, label in enumerate((click, both)):
        labels[mt, row:row + 1, :] = jnp.where(mine, jnp.concatenate([label] * tp, axis=1), 0.0)
    for copy in feat_copies + lab_copies:
        copy.start()
    for t in range(2):
        launch(t, 0, 1)
    feats[own_rows, :] = f_ref[...]
    for t in range(2):
        weights[t, block_rows(0), :] = w1_ref[t]

    span = 2
    while span * rows < 128 and span < dp:
        span *= 2
    started = [False, False]

    def multiply(t, group):
        place = pl.ds(pl.multiple_of((flip_rel(group * span) // span) * (span * rows), span * rows), span * rows)
        opening = not started[t]
        started[t] = True

        def one(j, carry):
            cols = pl.ds(pl.multiple_of(j * tile, tile), tile)
            value = jnp.dot(feats[:, place], weights[t, place, cols], preferred_element_type=F32)
            pre[t, :, cols] = value + (b1_ref[t:t + 1, cols] if opening else pre[t, :, cols])
            return carry

        lax.fori_loop(0, tiles, one, 0)

    waiting = [[t, group] for group in range(dp // span) for t in range(2)]
    arrived = [{0}, {0}]

    def advance(keep):
        for t, group in list(waiting):
            rels = range(group * span, (group + 1) * span)
            if all(rel & 1 or rel in arrived[t] for rel in rels) and len(waiting) > keep:
                for rel in rels:
                    if rel & 1:
                        gathers[t, rel].wait_recv()
                multiply(t, group)
                waiting.remove([t, group])

    for phase in range(len(high)):
        arriving = []
        for t in range(2):
            held = [0]
            for mask in orders[t][:phase]:
                held = held + [rel ^ mask for rel in held]
            arriving.append([rel ^ orders[t][phase] for rel in held])
        for step in range(len(arriving[0])):
            for t in range(2):
                rel = arriving[t][step]
                gathers[t, rel].wait_recv()
                for mask in orders[t][phase + 1:]:
                    launch(t, rel, mask)
                launch(t, rel, 1)
                arrived[t].add(rel)
        if phase == 0:
            for copy in feat_copies + lab_copies:
                copy.wait_recv()
            feats_t[...] = feats[...].T
            advance(2)
    advance(2)
    label_sum = labels[0]
    for j in range(1, tp):
        label_sum = label_sum + labels[j]
    label_y = label_sum[0:1]
    label_z = label_sum[1:2]
    for t, group in waiting:
        for rel in range(group * span + 1, (group + 1) * span, 2):
            gathers[t, rel].wait_recv()
        last = pl.ds(pl.multiple_of((flip_rel(group * span) // span) * (span * rows), span * rows), span * rows)

        def forward(j, total, t=t, last=last):
            cols = pl.ds(pl.multiple_of(j * tile, tile), tile)
            value = pre[t, :, cols] + jnp.dot(feats[:, last], weights[t, last, cols], preferred_element_type=F32)
            pre[t, :, cols] = value
            hidden = jnp.maximum(value, 0.0).astype(BF16)
            hid[t, :, cols] = hidden
            row = jnp.broadcast_to(w2_ref[t:t + 1, cols], (16, tile)).astype(BF16)
            return total + lax.dot_general(row, hidden, (((1,), (1,)), ((), ())), preferred_element_type=F32)

        total = lax.fori_loop(0, tiles, forward, jnp.zeros((16, count), F32))
        logit_out[t] = total[0:8]
    logit_copies = [to_tensor(j, 2, logit_out, logit_in.at[mt]) for j in range(1, tp)]
    for copy in logit_copies:
        copy.start()
    logit_in[mt] = logit_out[...]
    for copy in logit_copies:
        copy.wait_recv()
    first = logit_in[0, 0]
    second = logit_in[0, 1]
    for j in range(1, tp):
        first = first + logit_in[j, 0]
        second = second + logit_in[j, 1]
    sa, na = jax.nn.sigmoid(first), jax.nn.sigmoid(-first)
    sb, nb = jax.nn.sigmoid(second), jax.nn.sigmoid(-second)
    q = na + sa * nb
    rest = jnp.log(q)
    la, lna, lb = log_sigmoid(first), log_sigmoid(-first), log_sigmoid(second)
    losses = -(label_y * la + (1.0 - label_y) * lna) - (label_z * (la + lb) + (1.0 - label_z) * rest)
    part = jnp.zeros((1, own_count), F32)
    for j in range(tp):
        part = jnp.where(mt == j, losses[0:1, j * own_count:(j + 1) * own_count], part)
    loss_ref[...] = part
    shared = (1.0 - label_z) * (sa * sb / q)
    slopes = (
        -(label_y * na - (1.0 - label_y) * sa) - (label_z * na - shared * na),
        -(label_z * nb - shared * nb),
    )
    columns = [jnp.transpose(slope)[:, 0:1] for slope in slopes]
    for t in range(2):
        for j in range(tiles):
            cols = pl.ds(j * tile, tile)
            value = columns[t] * w2_ref[t:t + 1, cols].astype(F32)
            dh[t, :, cols] = jnp.where(pre[t, :, cols] > 0.0, value, 0.0).astype(BF16)

    def grad_block(t, rel):
        return jnp.dot(feats_t[block_rows(rel), :], dh[t], preferred_element_type=F32)

    scatters = {}

    def send_sum(t, key, mask, value):
        out_buf[t, key] = value.astype(BF16)
        copy = pltpu.make_async_remote_copy(
            src_ref=out_buf.at[t, key], dst_ref=in_buf.at[t, key],
            send_sem=ws_send.at[t, key], recv_sem=ws_recv.at[t, key],
            device_id={"dp": peer(mask)}, device_id_type=MESH,
        )
        copy.start()
        scatters[t, key] = copy

    ranked = []
    for t in range(2):
        ranked.append(sorted(range(0, dp, 2), key=lambda rel: (first_phase(rel, orders[t]), -bin(rel).count("1"))))

    def to_sibling(step):
        for t in range(2):
            rel = ranked[t][step]
            send_sum(t, rel ^ 1, 1, grad_block(t, rel ^ 1))

    def reduced(t, rel):
        value = grad_block(t, rel)
        keys = [rel ^ 1] + [rel ^ mask for mask in orders[t][:first_phase(rel, orders[t])]]
        for key in keys:
            scatters_recv(t, key)
            value = value + in_buf[t, key].astype(F32)
        return value

    def scatters_recv(t, key):
        pltpu.make_async_remote_copy(
            src_ref=out_buf.at[t, key], dst_ref=in_buf.at[t, key],
            send_sem=ws_send.at[t, key], recv_sem=ws_recv.at[t, key],
            device_id={"dp": peer(1)}, device_id_type=MESH,
        ).wait_recv()

    def process(step):
        for t in range(2):
            rel = ranked[t][step]
            if rel:
                mask = orders[t][first_phase(rel, orders[t])]
                send_sum(t, rel, mask, reduced(t, rel))
            else:
                value = reduced(t, 0) * scale
                for c in range(chunks):
                    gw_ref[pl.ds(2 * c + t, rows, stride=2 * chunks), :] = value[:, c * lanes:(c + 1) * lanes]

    lanes = gw_ref.shape[1]
    chunks = units // lanes
    early = dp // 4
    to_sibling(0)
    to_sibling(1)
    for step in range(early):
        process(step)
        if step + 2 < dp // 2:
            to_sibling(step + 2)
    for step in range(early + 2, dp // 2):
        to_sibling(step)

    def backward(j, carry):
        place = pl.ds(pl.multiple_of(j * tile, tile), tile)
        value = jnp.zeros((count, tile), F32)
        for t in range(2):
            value = value + lax.dot_general(
                dh[t], weights[t, place, :], (((1,), (1,)), ((), ())), preferred_element_type=F32
            )
        rows_out[:, place] = value.astype(BF16)
        return carry

    lax.fori_loop(0, width // tile, backward, 0)

    def rows_of(index):
        return pl.ds(pl.multiple_of(index * own_count, own_count), own_count)

    row_copies = [
        to_tensor(j, 3, rows_out.at[rows_of(lax.rem(mt + j, tp))], rows_in.at[j]) for j in range(1, tp)
    ]
    for copy in row_copies:
        copy.start()

    for t in range(2):
        for j in range(tiles):
            cols = pl.ds(j * tile, tile)
            sums[0, t:t + 1, cols] = jnp.sum(dh[t, :, cols].astype(F32), axis=0, keepdims=True)
            sums[0, 2 + t:3 + t, cols] = jnp.sum(columns[t] * hid[t, :, cols].astype(F32), axis=0, keepdims=True)
    masks = [1] + high
    sum_copies = []

    def exchange(phase):
        copy = pltpu.make_async_remote_copy(
            src_ref=sums.at[phase], dst_ref=sums_in.at[phase], send_sem=b_send.at[phase], recv_sem=b_recv.at[phase],
            device_id={"dp": peer(masks[phase])}, device_id_type=MESH,
        )
        copy.start()
        sum_copies.append(copy)

    def combine(phase):
        sum_copies[phase].wait_recv()
        sums[phase + 1] = sums[phase] + sums_in[phase]
        if phase + 1 < len(masks):
            exchange(phase + 1)

    exchange(0)
    for step in range(early, dp // 2 - 1):
        if step == early:
            combine(0)
        process(step)
    for phase in range(1, len(masks)):
        combine(phase)
    small_ref[0] = sums[len(masks), 0:2] * scale
    small_ref[1] = sums[len(masks), 2:4] * scale
    for copy in row_copies:
        copy.wait_recv()
    own = rows_out[rows_of(mt), :].astype(F32)
    for j in range(1, tp):
        own = own + rows_in[j].astype(F32)
    gf_ref[...] = own.astype(BF16)
    process(dp // 2 - 1)
    for copy in list(gathers.values()) + feat_copies + lab_copies + logit_copies + list(scatters.values()) + row_copies + sum_copies:
        copy.wait_send()


def write_out(loss, gf, gw, small, loss_out, gf_out, gw_out, bias_out, out_out, sems):
    pairs = (
        (gw, gw_out), (gf, gf_out), (loss, loss_out),
        (small.at[0], bias_out), (small.at[1], out_out),
    )
    copies = [pltpu.make_async_copy(src, dst, sems.at[i]) for i, (src, dst) in enumerate(pairs)]
    for copy in copies:
        copy.start()
    for copy in copies:
        copy.wait()


def solution(mesh):
    dp, tp = mesh.shape["dp"], mesh.shape["tensor"]

    def local(features, click, convert, w1, b1, w2):
        own_count, width = features.shape
        rows, _, units = w1.shape
        count = own_count * tp
        scale = 1.0 / math.sqrt(own_count * dp * tp)
        lanes = min(128, units)
        chunks = units // lanes
        vmem = pl.BlockSpec(memory_space=pltpu.VMEM)
        loss, gf, gw, small = pl.pallas_call(
            functools.partial(kernel, dp, tp, scale),
            out_shape=(
                jax.ShapeDtypeStruct((1, own_count), F32),
                jax.ShapeDtypeStruct((own_count, width), BF16),
                jax.ShapeDtypeStruct((rows * chunks * 2, lanes), F32),
                jax.ShapeDtypeStruct((2, 2, units), F32),
            ),
            in_specs=[vmem] * 6,
            out_specs=(vmem,) * 4,
            scratch_shapes=[
                pltpu.VMEM((2, width, units), BF16),
                pltpu.VMEM((count, width), BF16),
                pltpu.VMEM((width, count), BF16),
                pltpu.VMEM((tp, 2, count), F32),
                pltpu.VMEM((2, 8, count), F32),
                pltpu.VMEM((tp, 2, 8, count), F32),
                pltpu.VMEM((2, count, units), F32),
                pltpu.VMEM((2, count, units), BF16),
                pltpu.VMEM((2, count, units), BF16),
                pltpu.VMEM((2, dp, rows, units), BF16),
                pltpu.VMEM((2, dp, rows, units), BF16),
                pltpu.VMEM((count, width), BF16),
                pltpu.VMEM((tp, own_count, width), BF16),
                pltpu.VMEM((dp.bit_length(), 4, units), F32),
                pltpu.VMEM((dp.bit_length(), 4, units), F32),
                pltpu.SemaphoreType.DMA((2, dp)),
                pltpu.SemaphoreType.DMA((2, dp)),
                pltpu.SemaphoreType.DMA((2, dp)),
                pltpu.SemaphoreType.DMA((2, dp)),
                pltpu.SemaphoreType.DMA((4, tp)),
                pltpu.SemaphoreType.DMA((4, tp)),
                pltpu.SemaphoreType.DMA((dp,)),
                pltpu.SemaphoreType.DMA((dp,)),
            ],
            compiler_params=pltpu.CompilerParams(
                collective_id=0, has_side_effects=True, vmem_limit_bytes=48 * 1024 * 1024
            ),
        )(features, click.reshape(1, own_count), convert.reshape(1, own_count), jnp.transpose(w1, (1, 0, 2)), b1, w2)
        anywhere = pl.BlockSpec(memory_space=pl.ANY)
        losses, gf, gw, bias, out = pl.pallas_call(
            write_out,
            out_shape=(
                jax.ShapeDtypeStruct(loss.shape, F32),
                jax.ShapeDtypeStruct(gf.shape, BF16),
                jax.ShapeDtypeStruct(gw.shape, F32),
                jax.ShapeDtypeStruct((2, units), F32),
                jax.ShapeDtypeStruct((2, units), F32),
            ),
            in_specs=[vmem] * 4,
            out_specs=(anywhere,) * 5,
            scratch_shapes=[pltpu.SemaphoreType.DMA((5,))],
            compiler_params=pltpu.CompilerParams(vmem_limit_bytes=4 * 1024 * 1024),
        )(loss, gf, gw, small)
        grad_w1 = gw.reshape(rows, chunks, 2, lanes).transpose(0, 2, 1, 3).reshape(rows, 2, units)
        return (losses.reshape(own_count), gf, grad_w1, bias, out)

    return jax.shard_map(
        local,
        mesh=mesh,
        in_specs=(
            P(("dp", "tensor"), None),
            P(("dp", "tensor")),
            P(("dp", "tensor")),
            P("dp", None, "tensor"),
            P(None, "tensor"),
            P(None, "tensor"),
        ),
        out_specs=(
            P(("dp", "tensor")),
            P(("dp", "tensor"), None),
            P("dp", None, "tensor"),
            P(None, "tensor"),
            P(None, "tensor"),
        ),
        check_vma=False,
    )
```

```python
import functools
import math

import jax
import jax.numpy as jnp
from jax import lax
from jax.experimental import pallas as pl
from jax.experimental.pallas import tpu as pltpu
from jax.sharding import PartitionSpec as P

MESH = pl.DeviceIdType.MESH
F32 = jnp.float32
BF16 = jnp.bfloat16


def log_sigmoid(x):
    return jnp.minimum(x, 0.0) - jnp.log1p(jnp.exp(-jnp.abs(x)))


def first_phase(rel, order):
    for phase, mask in enumerate(order):
        if rel & mask:
            return phase
    return len(order)


def kernel(
    dp, tp, scale, f_hbm, click_hbm, convert_hbm, w1_ref, b1_hbm, w2_hbm,
    loss_ref, gf_ref, gw_ref, small_ref,
    weights, feats, feats_t, labels, logit_out, logit_in, pre, hid, dh,
    out_buf, in_buf, rows_out, rows_in, sums, sums_in,
    click_ref, convert_ref, b1_ref, w2_ref, in_sems,
    wg_send, wg_recv, ws_send, ws_recv, t_send, t_recv, b_send, b_recv,
):
    me = lax.axis_index("dp")
    mt = lax.axis_index("tensor")
    rows, units = w1_ref.shape[1], w1_ref.shape[2]
    own_count, width = f_hbm.shape
    count = own_count * tp
    tile = min(256, units)
    tiles = units // tile
    high = [1 << bit for bit in range(1, dp.bit_length() - 1)]
    orders = (high, high[::-1])

    def flip(mask):
        return me + mask - 2 * (me & mask)

    def flip_rel(rel):
        out = me
        bit = 1
        while bit <= rel:
            if rel & bit:
                out = out + bit - 2 * (lax.rem(me // bit, 2) * bit)
            bit *= 2
        return out

    def peer(rel):
        return flip_rel(rel)

    barrier = pltpu.get_barrier_semaphore()
    for j in range(1, tp):
        pl.semaphore_signal(barrier, inc=1, device_id={"tensor": lax.rem(mt + j, tp)}, device_id_type=MESH)
    for mask in high + [1]:
        pl.semaphore_signal(barrier, inc=1, device_id={"dp": peer(mask)}, device_id_type=MESH)
    own_rows = pl.ds(pl.multiple_of(mt * own_count, own_count), own_count)
    loads = [
        pltpu.make_async_copy(src, dst, in_sems.at[i])
        for i, (src, dst) in enumerate((
            (f_hbm, feats.at[own_rows]), (click_hbm, click_ref), (convert_hbm, convert_ref),
            (b1_hbm, b1_ref), (w2_hbm, w2_ref),
        ))
    ]
    for copy in loads:
        copy.start()
    pl.semaphore_wait(barrier, len(high) + tp)

    def block_rows(rel):
        return pl.ds(pl.multiple_of(flip_rel(rel) * rows, rows), rows)

    def gather_copy(t, rel, mask):
        place = weights.at[t, block_rows(rel)]
        src = w1_ref.at[t] if rel == 0 else place
        key = rel ^ mask
        return pltpu.make_async_remote_copy(
            src_ref=src, dst_ref=place, send_sem=wg_send.at[t, key], recv_sem=wg_recv.at[t, key],
            device_id={"dp": peer(mask)}, device_id_type=MESH,
        )

    def to_tensor(j, kind, src, dst):
        return pltpu.make_async_remote_copy(
            src_ref=src, dst_ref=dst, send_sem=t_send.at[kind, j], recv_sem=t_recv.at[kind, j],
            device_id={"tensor": lax.rem(mt + j, tp)}, device_id_type=MESH,
        )

    pending = []
    gathers = {}

    def launch(t, rel, mask):
        copy = gather_copy(t, rel, mask)
        copy.start()
        gathers[t, rel ^ mask] = copy

    for phase in range(len(high)):
        for t in range(2):
            launch(t, 0, orders[t][phase])
    for copy in loads:
        copy.wait()
    feat_copies = [to_tensor(j, 0, feats.at[own_rows], feats.at[own_rows]) for j in range(1, tp)]
    for copy in feat_copies:
        copy.start()
    lab_copies = [to_tensor(j, 1, labels.at[mt], labels.at[mt]) for j in range(1, tp)]
    click = click_ref[...].astype(F32)
    both = click * convert_ref[...].astype(F32)
    mine = lax.broadcasted_iota(jnp.int32, (1, count), 1) // own_count == mt
    for row, label in enumerate((click, both)):
        labels[mt, row:row + 1, :] = jnp.where(mine, jnp.concatenate([label] * tp, axis=1), 0.0)
    for copy in lab_copies:
        copy.start()
    for t in range(2):
        launch(t, 0, 1)
    for t in range(2):
        weights[t, block_rows(0), :] = w1_ref[t]

    span = 2
    while span * rows < 128 and span < dp:
        span *= 2
    started = [False, False]

    def multiply(t, group):
        place = pl.ds(pl.multiple_of((flip_rel(group * span) // span) * (span * rows), span * rows), span * rows)
        multiply_rows(t, place)

    def multiply_rows(t, place):
        opening = not started[t]
        started[t] = True

        def one(j, carry):
            cols = pl.ds(pl.multiple_of(j * tile, tile), tile)
            value = jnp.dot(feats[:, place], weights[t, place, cols], preferred_element_type=F32)
            pre[t, :, cols] = value + (b1_ref[t:t + 1, cols] if opening else pre[t, :, cols])
            return carry

        lax.fori_loop(0, tiles, one, 0)

    waiting = [[t, group] for group in range(dp // span) for t in range(2)]
    arrived = [{0}, {0}]

    def advance(keep):
        for t, group in list(waiting):
            rels = range(group * span, (group + 1) * span)
            if all(rel & 1 or rel in arrived[t] for rel in rels) and len(waiting) > keep:
                for rel in rels:
                    if rel & 1:
                        gathers[t, rel].wait_recv()
                multiply(t, group)
                waiting.remove([t, group])

    for phase in range(len(high)):
        arriving = []
        for t in range(2):
            held = [0]
            for mask in orders[t][:phase]:
                held = held + [rel ^ mask for rel in held]
            arriving.append([rel ^ orders[t][phase] for rel in held])
        for step in range(len(arriving[0])):
            for t in range(2):
                rel = arriving[t][step]
                gathers[t, rel].wait_recv()
                for mask in orders[t][phase + 1:]:
                    launch(t, rel, mask)
                launch(t, rel, 1)
                arrived[t].add(rel)
        if phase == 0:
            for copy in feat_copies + lab_copies:
                copy.wait_recv()
            feats_t[...] = feats[...].T
            advance(2)
    advance(2)
    label_sum = labels[0]
    for j in range(1, tp):
        label_sum = label_sum + labels[j]
    label_y = label_sum[0:1]
    label_z = label_sum[1:2]
    def place_of(rel):
        return pl.ds(pl.multiple_of(flip_rel(rel) * rows, rows), rows)

    split = span == 2 and rows % 128 == 0
    if split:
        for t, group in waiting:
            multiply_rows(t, place_of(group * span))
    for t, group in waiting:
        for rel in range(group * span + 1, (group + 1) * span, 2):
            gathers[t, rel].wait_recv()
        last = place_of(group * span + 1) if split else pl.ds(pl.multiple_of((flip_rel(group * span) // span) * (span * rows), span * rows), span * rows)

        def forward(j, total, t=t, last=last):
            cols = pl.ds(pl.multiple_of(j * tile, tile), tile)
            value = pre[t, :, cols] + jnp.dot(feats[:, last], weights[t, last, cols], preferred_element_type=F32)
            pre[t, :, cols] = value
            hidden = jnp.maximum(value, 0.0).astype(BF16)
            hid[t, :, cols] = hidden
            row = jnp.broadcast_to(w2_ref[t:t + 1, cols], (16, tile)).astype(BF16)
            return total + lax.dot_general(row, hidden, (((1,), (1,)), ((), ())), preferred_element_type=F32)

        total = lax.fori_loop(0, tiles, forward, jnp.zeros((16, count), F32))
        logit_out[t:t + 1, :] = total[0:1]
    logit_copies = [to_tensor(j, 2, logit_out, logit_in.at[mt]) for j in range(1, tp)]
    for copy in logit_copies:
        copy.start()
    logit_in[mt] = logit_out[...]
    for copy in logit_copies:
        copy.wait_recv()
    first = logit_in[0, 0:1]
    second = logit_in[0, 1:2]
    for j in range(1, tp):
        first = first + logit_in[j, 0:1]
        second = second + logit_in[j, 1:2]
    sa, na = jax.nn.sigmoid(first), jax.nn.sigmoid(-first)
    sb, nb = jax.nn.sigmoid(second), jax.nn.sigmoid(-second)
    q = na + sa * nb
    rest = jnp.log(q)
    la, lna, lb = log_sigmoid(first), log_sigmoid(-first), log_sigmoid(second)
    losses = -(label_y * la + (1.0 - label_y) * lna) - (label_z * (la + lb) + (1.0 - label_z) * rest)
    part = jnp.zeros((1, own_count), F32)
    for j in range(tp):
        part = jnp.where(mt == j, losses[0:1, j * own_count:(j + 1) * own_count], part)
    loss_ref[...] = part
    shared = (1.0 - label_z) * (sa * sb / q)
    slopes = (
        -(label_y * na - (1.0 - label_y) * sa) - (label_z * na - shared * na),
        -(label_z * nb - shared * nb),
    )
    columns = [jnp.transpose(jnp.broadcast_to(slope, (8, count)))[:, 0:1] for slope in slopes]
    def slope_rows(t):
        for j in range(tiles):
            cols = pl.ds(j * tile, tile)
            value = columns[t] * w2_ref[t:t + 1, cols].astype(F32)
            dh[t, :, cols] = jnp.where(pre[t, :, cols] > 0.0, value, 0.0).astype(BF16)

    def grad_block(t, rel):
        return jnp.dot(feats_t[block_rows(rel), :], dh[t], preferred_element_type=F32)

    scatters = {}

    def send_sum(t, key, mask, value):
        out_buf[t, key] = value.astype(BF16)
        copy = pltpu.make_async_remote_copy(
            src_ref=out_buf.at[t, key], dst_ref=in_buf.at[t, key],
            send_sem=ws_send.at[t, key], recv_sem=ws_recv.at[t, key],
            device_id={"dp": peer(mask)}, device_id_type=MESH,
        )
        copy.start()
        scatters[t, key] = copy

    ranked = []
    for t in range(2):
        ranked.append(sorted(range(0, dp, 2), key=lambda rel: (first_phase(rel, orders[t]), -bin(rel).count("1"))))

    def to_sibling(step):
        for t in range(2):
            rel = ranked[t][step]
            if step == 0:
                slope_rows(t)
            send_sum(t, rel ^ 1, 1, grad_block(t, rel ^ 1))

    def reduced(t, rel):
        value = grad_block(t, rel)
        keys = [rel ^ 1] + [rel ^ mask for mask in orders[t][:first_phase(rel, orders[t])]]
        for key in keys:
            scatters_recv(t, key)
            value = value + in_buf[t, key].astype(F32)
        return value

    def scatters_recv(t, key):
        pltpu.make_async_remote_copy(
            src_ref=out_buf.at[t, key], dst_ref=in_buf.at[t, key],
            send_sem=ws_send.at[t, key], recv_sem=ws_recv.at[t, key],
            device_id={"dp": peer(1)}, device_id_type=MESH,
        ).wait_recv()

    def process(step):
        for t in range(2):
            rel = ranked[t][step]
            if rel:
                mask = orders[t][first_phase(rel, orders[t])]
                send_sum(t, rel, mask, reduced(t, rel))
            else:
                value = reduced(t, 0) * scale
                for c in range(chunks):
                    gw_ref[pl.ds(2 * c + t, rows, stride=2 * chunks), :] = value[:, c * lanes:(c + 1) * lanes]

    lanes = gw_ref.shape[1]
    chunks = units // lanes
    early = dp // 4
    to_sibling(0)
    to_sibling(1)
    for step in range(early):
        process(step)
        if step + 2 < dp // 2:
            to_sibling(step + 2)
    for step in range(early + 2, dp // 2):
        to_sibling(step)

    def backward(j, carry):
        place = pl.ds(pl.multiple_of(j * tile, tile), tile)
        value = jnp.zeros((count, tile), F32)
        for t in range(2):
            value = value + lax.dot_general(
                dh[t], weights[t, place, :], (((1,), (1,)), ((), ())), preferred_element_type=F32
            )
        rows_out[:, place] = value.astype(BF16)
        return carry

    lax.fori_loop(0, width // tile, backward, 0)

    def rows_of(index):
        return pl.ds(pl.multiple_of(index * own_count, own_count), own_count)

    row_copies = [
        to_tensor(j, 3, rows_out.at[rows_of(lax.rem(mt + j, tp))], rows_in.at[j]) for j in range(1, tp)
    ]
    for copy in row_copies:
        copy.start()

    for t in range(2):
        for j in range(tiles):
            cols = pl.ds(j * tile, tile)
            sums[0, t:t + 1, cols] = jnp.sum(dh[t, :, cols].astype(F32), axis=0, keepdims=True)
            sums[0, 2 + t:3 + t, cols] = jnp.sum(columns[t] * hid[t, :, cols].astype(F32), axis=0, keepdims=True)
    masks = [1] + high
    sum_copies = []

    def exchange(phase):
        copy = pltpu.make_async_remote_copy(
            src_ref=sums.at[phase], dst_ref=sums_in.at[phase], send_sem=b_send.at[phase], recv_sem=b_recv.at[phase],
            device_id={"dp": peer(masks[phase])}, device_id_type=MESH,
        )
        copy.start()
        sum_copies.append(copy)

    def combine(phase):
        sum_copies[phase].wait_recv()
        sums[phase + 1] = sums[phase] + sums_in[phase]
        if phase + 1 < len(masks):
            exchange(phase + 1)

    exchange(0)
    for step in range(early, dp // 2 - 1):
        if step == early:
            combine(0)
        process(step)
    for phase in range(1, len(masks)):
        combine(phase)
    small_ref[0] = sums[len(masks), 0:2] * scale
    small_ref[1] = sums[len(masks), 2:4] * scale
    for copy in row_copies:
        copy.wait_recv()
    own = rows_out[rows_of(mt), :].astype(F32)
    for j in range(1, tp):
        own = own + rows_in[j].astype(F32)
    gf_ref[...] = own.astype(BF16)
    process(dp // 2 - 1)
    for copy in list(gathers.values()) + feat_copies + lab_copies + logit_copies + list(scatters.values()) + row_copies + sum_copies:
        copy.wait_send()


def write_out(loss, gf, gw, small, loss_out, gf_out, gw_out, bias_out, out_out, sems):
    pairs = (
        (gw, gw_out), (gf, gf_out), (loss, loss_out),
        (small.at[0], bias_out), (small.at[1], out_out),
    )
    copies = [pltpu.make_async_copy(src, dst, sems.at[i]) for i, (src, dst) in enumerate(pairs)]
    for copy in copies:
        copy.start()
    for copy in copies:
        copy.wait()


def solution(mesh):
    dp, tp = mesh.shape["dp"], mesh.shape["tensor"]

    def local(features, click, convert, w1, b1, w2):
        own_count, width = features.shape
        rows, _, units = w1.shape
        count = own_count * tp
        scale = 1.0 / math.sqrt(own_count * dp * tp)
        lanes = min(128, units)
        chunks = units // lanes
        vmem = pl.BlockSpec(memory_space=pltpu.VMEM)
        hbm = pl.BlockSpec(memory_space=pltpu.HBM)
        loss, gf, gw, small = pl.pallas_call(
            functools.partial(kernel, dp, tp, scale),
            out_shape=(
                jax.ShapeDtypeStruct((1, own_count), F32),
                jax.ShapeDtypeStruct((own_count, width), BF16),
                jax.ShapeDtypeStruct((rows * chunks * 2, lanes), F32),
                jax.ShapeDtypeStruct((2, 2, units), F32),
            ),
            in_specs=[hbm, hbm, hbm, vmem, hbm, hbm],
            out_specs=(vmem,) * 4,
            scratch_shapes=[
                pltpu.VMEM((2, width, units), BF16),
                pltpu.VMEM((count, width), BF16),
                pltpu.VMEM((width, count), BF16),
                pltpu.VMEM((tp, 2, count), F32),
                pltpu.VMEM((2, count), F32),
                pltpu.VMEM((tp, 2, count), F32),
                pltpu.VMEM((2, count, units), F32),
                pltpu.VMEM((2, count, units), BF16),
                pltpu.VMEM((2, count, units), BF16),
                pltpu.VMEM((2, dp, rows, units), BF16),
                pltpu.VMEM((2, dp, rows, units), BF16),
                pltpu.VMEM((count, width), BF16),
                pltpu.VMEM((tp, own_count, width), BF16),
                pltpu.VMEM((dp.bit_length(), 4, units), F32),
                pltpu.VMEM((dp.bit_length(), 4, units), F32),
                pltpu.VMEM((1, own_count), jnp.int32),
                pltpu.VMEM((1, own_count), jnp.int32),
                pltpu.VMEM((2, units), F32),
                pltpu.VMEM((2, units), BF16),
                pltpu.SemaphoreType.DMA((5,)),
                pltpu.SemaphoreType.DMA((2, dp)),
                pltpu.SemaphoreType.DMA((2, dp)),
                pltpu.SemaphoreType.DMA((2, dp)),
                pltpu.SemaphoreType.DMA((2, dp)),
                pltpu.SemaphoreType.DMA((4, tp)),
                pltpu.SemaphoreType.DMA((4, tp)),
                pltpu.SemaphoreType.DMA((dp,)),
                pltpu.SemaphoreType.DMA((dp,)),
            ],
            compiler_params=pltpu.CompilerParams(
                collective_id=0, has_side_effects=True, vmem_limit_bytes=48 * 1024 * 1024
            ),
        )(features, click.reshape(1, own_count), convert.reshape(1, own_count), jnp.transpose(w1, (1, 0, 2)), b1, w2)
        anywhere = pl.BlockSpec(memory_space=pl.ANY)
        losses, gf, gw, bias, out = pl.pallas_call(
            write_out,
            out_shape=(
                jax.ShapeDtypeStruct(loss.shape, F32),
                jax.ShapeDtypeStruct(gf.shape, BF16),
                jax.ShapeDtypeStruct(gw.shape, F32),
                jax.ShapeDtypeStruct((2, units), F32),
                jax.ShapeDtypeStruct((2, units), F32),
            ),
            in_specs=[vmem] * 4,
            out_specs=(anywhere,) * 5,
            scratch_shapes=[pltpu.SemaphoreType.DMA((5,))],
            compiler_params=pltpu.CompilerParams(vmem_limit_bytes=4 * 1024 * 1024),
        )(loss, gf, gw, small)
        grad_w1 = gw.reshape(rows, chunks, 2, lanes).transpose(0, 2, 1, 3).reshape(rows, 2, units)
        return (losses.reshape(own_count), gf, grad_w1, bias, out)

    return jax.shard_map(
        local,
        mesh=mesh,
        in_specs=(
            P(("dp", "tensor"), None),
            P(("dp", "tensor")),
            P(("dp", "tensor")),
            P("dp", None, "tensor"),
            P(None, "tensor"),
            P(None, "tensor"),
        ),
        out_specs=(
            P(("dp", "tensor")),
            P(("dp", "tensor"), None),
            P("dp", None, "tensor"),
            P(None, "tensor"),
            P(None, "tensor"),
        ),
        check_vma=False,
    )
```
